32 devices in a mesh: fsdp: 2 (over y), tensor: 16 (over z, x, core).
Axes of the slice: x: 2, y: 2, z: 4, core: 2. Of those that a mesh axis runs over, the one named last changes fastest.
Arguments:
- momentum: bfloat16 [8192, 28672], P('fsdp', 'tensor'), may hold values from -6 to 6
- gradient: bfloat16 [8192, 28672], P('fsdp', 'tensor'), may hold values from -4 to 4
- factor: float32 [28672, 512], P('tensor', 'fsdp'), may hold values from -0.03125 to 0.03125
Outputs:
- new_momentum: bfloat16 [8192, 28672], P('fsdp', 'tensor')
- new_factor: float32 [28672, 512], P('tensor', 'fsdp')
- update: bfloat16 [8192, 28672], P('fsdp', 'tensor')
The draws below stay inside these ranges and needn't reach their ends.
All inputs are finite; a program needn't handle non-finite values.
Results may differ from the reference program's by a relative error of at most 0.017.
Values may be sent and summed in bfloat16 or wider, within the bound.
A program may use at most 128 MiB of HBM per device.

```python
import jax
import jax.numpy as jnp
from jax import lax

D = 8192
FF = 28672
R = 512


def steps_of(own_key, shape, shards, smallest, top_value):
    level = 1.0
    for dim, parts in shards:
        heights = jax.random.uniform(jax.random.fold_in(jax.random.fold_in(own_key, 6), dim), (parts,), jnp.float32, smallest / len(shards), top_value / len(shards))
        level = level * jnp.repeat(jnp.exp(heights), shape[dim] // parts).reshape((-1,) + (1,) * (len(shape) - 1 - dim))
    return level


def noise(own_key, extent, scale, most, pieces=(), held_as=jnp.bfloat16):
    result = jax.random.normal(own_key, extent, jnp.float32) * scale
    if len(pieces) > 0:
        result = steps_of(own_key, extent, pieces, -0.22, 0.18) * result
    return jnp.clip(result, min=-most, max=most).astype(held_as)


def setup_inputs(seed: int = 0) -> dict:
    splits = jax.random.split(jax.random.key(seed), 4)
    momentum = noise(splits[0], (D, FF), 1.0, 6.0, ((0, 2), (1, 16)))
    gradient = noise(splits[1], (D, FF), 0.5, 4.0, ((0, 2), (1, 16)))
    factor = noise(splits[2], (FF, R), FF ** -0.5, 0.03125, ((0, 16), (1, 2)), jnp.float32)
    return dict(momentum=momentum, gradient=gradient, factor=factor)


decay_rate = 0.95
epsilon = 1e-06

def reference(momentum, gradient, factor):
    blended = (momentum.astype(jnp.float32) + gradient.astype(jnp.float32)).astype(jnp.bfloat16)
    lowered = factor.astype(jnp.bfloat16)
    left_factor = jnp.dot(blended.astype(jnp.float32), lowered.astype(jnp.float32), preferred_element_type=jnp.float32)
    gram_matrix = lax.dot_general(left_factor, left_factor, (((0,), (0,)), ((), ())), precision=lax.Precision.HIGHEST)
    lower_factor = jnp.linalg.cholesky(gram_matrix)
    solved = jax.scipy.linalg.solve_triangular(lower_factor, left_factor.T, lower=True)
    orthonormal = solved.T.astype(jnp.bfloat16)
    right_factor = lax.dot_general(blended.astype(jnp.float32), orthonormal.astype(jnp.float32), (((0,), (0,)), ((), ())), preferred_element_type=jnp.float32)
    inverse = lax.rsqrt(lax.optimization_barrier(jnp.sum(right_factor * right_factor, axis=0)) + epsilon)
    new_factor = right_factor * inverse[None, :]
    product = lax.dot_general(orthonormal.astype(jnp.float32), right_factor.astype(jnp.bfloat16).astype(jnp.float32), (((1,), (1,)), ((), ())), preferred_element_type=jnp.float32)
    new_momentum = (blended.astype(jnp.float32) - (1.0 - decay_rate) * product).astype(jnp.bfloat16)
    stepped = lax.dot_general(orthonormal.astype(jnp.float32), new_factor.astype(jnp.bfloat16).astype(jnp.float32), (((1,), (1,)), ((), ())), preferred_element_type=jnp.float32)
    update = (stepped * jnp.sqrt(jnp.float32(D * FF / R))).astype(jnp.bfloat16)
    return (new_momentum, new_factor, update)
```

```python
import functools

import jax
import jax.numpy as jnp
from jax import lax
from jax.experimental import pallas as pl
from jax.experimental.pallas import tpu as pltpu
from jax.sharding import PartitionSpec as P

decay_rate = 0.95
epsilon = 1e-06
BLOCK = 128
HALF = 64
MESH = pl.DeviceIdType.MESH
F32 = jnp.float32
BF16 = jnp.bfloat16


def inverse_kernel(gram_ref, high_ref, low_ref, state):
    rank = gram_ref.shape[0]
    iota = functools.partial(lax.broadcasted_iota, jnp.int32)
    same = iota((rank, rank), 0) == iota((rank, rank), 1)
    diagonal = jnp.where(same, gram_ref[...], 0.0)
    scale_row = 1.0 / jnp.sqrt(jnp.sum(diagonal, axis=0, keepdims=True))
    scale_column = 1.0 / jnp.sqrt(jnp.sum(diagonal, axis=1, keepdims=True))
    state[...] = gram_ref[...] * scale_row * scale_column
    row = iota((HALF, BLOCK), 0)
    lane = iota((HALF, BLOCK), 1)
    wide_row = iota((HALF, rank), 0)
    wide = iota((HALF, rank), 1)
    exact = dict(precision=lax.Precision.HIGHEST, preferred_element_type=F32)
    over = (((0,), (0,)), ((), ()))

    @pl.loop(0, rank // HALF)
    def _(b):
        at = pl.multiple_of(b * HALF, HALF)
        tile = pl.multiple_of(b // 2 * BLOCK, BLOCK)
        odd = lax.rem(b, 2) == 1
        square = state[pl.ds(at, HALF), pl.ds(tile, BLOCK)]
        square = jnp.where(odd, pltpu.roll(square, HALF, 1), square)
        a = jnp.where(lane < HALF, square, (lane - HALF == row).astype(F32))
        for base in range(0, HALF, 8):
            now = a[base:]
            spread = [
                jnp.broadcast_to(now[:, base + k : base + k + 1], now.shape) for k in range(8)
            ]
            for k in range(0, 8 if base + 8 < HALF else 6, 2):
                first, second = spread[k], spread[k + 1]
                p = first[k : k + 1]
                q = second[k : k + 1]
                r = second[k + 1 : k + 2]
                inverse = 1.0 / (p * r - q * q)
                below = row[: HALF - base] > k + 1
                one = jnp.where(below, (first * r - second * q) * inverse, 0.0)
                two = jnp.where(below, (second * p - first * q) * inverse, 0.0)
                for n in range(k + 2, 8):
                    old = spread[n]
                    spread[n] = old - one * old[k : k + 1] - two * old[k + 1 : k + 2]
                now = now - one * now[k : k + 1] - two * now[k + 1 : k + 2]
            a = now if base == 0 else jnp.concatenate([a[:base], now], axis=0)
        above = pltpu.roll(a, 1, 0)
        left_of = lane == row - 1
        edge = jnp.sum(jnp.where(left_of, a, 0.0), axis=1, keepdims=True)
        corner = jnp.sum(jnp.where(left_of, above, 0.0), axis=1, keepdims=True)
        odd_row = lax.rem(row, 2) == 1
        a = a - jnp.where(odd_row, edge / jnp.where(odd_row, corner, 1.0), 0.0) * above
        pivots = jnp.sum(jnp.where(lane == row, a, 0.0), axis=1, keepdims=True)
        block_inverse = pltpu.roll(a * (1.0 / jnp.sqrt(pivots)), HALF, 1)[:, :HALF]
        inside = (wide >= at) & (wide < at + HALF)
        rows = jnp.where(inside, (wide - at == wide_row).astype(F32), state[pl.ds(at, HALF), :])
        solved = jnp.dot(block_inverse, rows, **exact)
        state[pl.ds(at, HALF), :] = solved
        result = jnp.where(wide < at + HALF, solved, 0.0) * scale_row
        high = result.astype(BF16)
        high_ref[pl.ds(at, HALF), :] = high
        low_ref[pl.ds(at, HALF), :] = (result - high.astype(F32)).astype(BF16)

        @pl.when(jnp.logical_not(odd))
        def _():
            later = pl.ds(pl.multiple_of(at + HALF, HALF), HALF)
            upper = pltpu.roll(state[pl.ds(at, HALF), pl.ds(tile, BLOCK)], HALF, 1)[:, :HALF]
            old = jnp.where(inside, 0.0, state[later, :])
            state[later, :] = old - lax.dot_general(upper, solved, over, **exact)

        for bb in range(rank // BLOCK - 1):

            @pl.when(b == 2 * bb + 1)
            def _():
                start, rest = bb * BLOCK, (bb + 1) * BLOCK
                pair = state[start:rest, :]
                r2 = iota(pair.shape, 0)
                c2 = iota(pair.shape, 1) - start
                dead = (r2 < HALF) & (c2 >= HALF) & (c2 < BLOCK)
                c3 = iota((rank - rest, rank), 1) - start
                old = jnp.where((c3 >= 0) & (c3 < BLOCK), 0.0, state[rest:, :])
                state[rest:, :] = old - lax.dot_general(
                    pair[:, rest:], jnp.where(dead, 0.0, pair), over, **exact
                )


def inverse_of_lower(gram):
    rank = gram.shape[0]
    vmem = pl.BlockSpec(memory_space=pltpu.VMEM)
    return pl.pallas_call(
        inverse_kernel,
        out_shape=(jax.ShapeDtypeStruct((rank, rank), BF16),) * 2,
        in_specs=[vmem],
        out_specs=(vmem, vmem),
        scratch_shapes=[pltpu.VMEM((rank, rank), F32)],
        compiler_params=pltpu.CompilerParams(vmem_limit_bytes=32 << 20),
        cost_estimate=pl.CostEstimate(flops=40_000_000_000, bytes_accessed=2 << 20, transcendentals=0),
        name="inverse",
    )(gram)


def butterfly(value, axis, size):
    if size & (size - 1):
        return lax.psum(value, axis)
    step = 1
    while step < size:
        value = value + lax.ppermute(value, axis, [(i, i ^ step) for i in range(size)])
        step *= 2
    return value


def left_kernel(
    nz,
    momentum,
    gradient,
    factor,
    blended_out,
    left_out,
    gram_out,
    w_out,
    lows,
    blended,
    stream_m,
    stream_g,
    part,
    got_a,
    sent_b,
    kept,
    got_b,
    sent_c,
    got_c,
    own,
    partial,
    left,
    w,
    gram,
    got_gram,
    in_sem,
    out_sem,
    l_sem,
    a_sem,
    b_sem,
    c_sem,
    d_sem,
    e_sem,
    f_sem,
    g_sem,
    k_sem,
):
    place = lax.axis_index("fsdp")
    t = lax.axis_index("tensor")
    c = lax.rem(t, 2)
    x = lax.rem(t // 2, 2)
    z = t // 4
    size = blended.shape[0] // (4 * nz)
    columns = w.shape[1]
    slots = stream_m.shape[0]
    per_half = columns // BLOCK
    groups = 2 * per_half
    near = range(per_half)
    far = range(per_half, groups)

    def at(zz, xx, cc):
        return place, (zz * 2 + xx) * 2 + cc

    def turned(d):
        return lax.rem(z + d, nz)

    def rows_of(cc, xx, zz):
        return pl.ds(pl.multiple_of(((cc * 2 + xx) * nz + zz) * size, size), size)

    y_peer = (1 - place, t)
    c_peer = at(z, x, 1 - c)
    x_peer = at(z, 1 - x, c)
    peers = [y_peer, c_peer, x_peer] + [at(turned(d), x, c) for d in range(1, nz)]

    def send(src, dst, sems, index, peer):
        return pltpu.make_async_remote_copy(
            src_ref=src,
            dst_ref=dst,
            send_sem=sems.at[(0,) + index],
            recv_sem=sems.at[(1,) + index],
            device_id=peer,
            device_id_type=MESH,
        )

    def position(i):
        quarter, j = i // nz, lax.rem(i, nz)
        cc = jnp.where(quarter < 2, 1 - c, c)
        xx = jnp.where(lax.rem(quarter, 2) == 0, 1 - x, x)
        return rows_of(cc, xx, lax.rem(z + 1 + j, nz))

    def fetch(i, slot):
        here = position(i)
        return (
            pltpu.make_async_copy(momentum.at[here], stream_m.at[slot], in_sem.at[0, slot]),
            pltpu.make_async_copy(gradient.at[here], stream_g.at[slot], in_sem.at[1, slot]),
        )

    chunks = 4 * nz
    for i in range(slots):
        for copy in fetch(i, i):
            copy.start()

    barrier = pltpu.get_barrier_semaphore()
    for peer in peers:
        pl.semaphore_signal(barrier, inc=1, device_id=peer, device_id_type=MESH)
    lows[0] = factor[...].astype(BF16)
    pl.semaphore_wait(barrier, len(peers))

    width = blended.shape[1]
    cut = width // 256 * 5 // 7 * 256
    pieces = (pl.ds(0, cut), pl.ds(cut, width - cut))

    def copy_l(k):
        return send(lows.at[0, pieces[k]], lows.at[1, pieces[k]], l_sem, (k,), y_peer)

    for k in range(2):
        copy_l(k).start()

    def copy_a(q, i):
        return send(part.at[q, i], got_a.at[q, i], a_sem, (q, i), c_peer)

    def copy_b(q, j):
        return send(sent_b.at[q, j], got_b.at[q, j], b_sem, (q, j), x_peer)

    def copy_c(q, d):
        return send(sent_c.at[q, d - 1], got_c.at[q, d - 1], c_sem, (q, d - 1), at(turned(d), x, c))

    def half(q):
        return place if q < per_half else 1 - place

    def spot(q):
        return half(q) * per_half + q % per_half

    def block(q, cc, xx, zz):
        return left.at[spot(q), rows_of(cc, xx, zz)]

    def copy_d(q, way, k):
        zz, to = (z - k, z + 1) if way == 0 else (z + k, z - 1)
        here = block(q, c, x, zz)
        return send(here, here, d_sem, (q, way, k), at(to, x, c))

    def can_send(way, k):
        return (z >= k) & (z < nz - 1) if way == 0 else (z + k < nz) & (z > 0)

    def copy_e(q, zz):
        here = block(q, c, x, zz)
        return send(here, here, e_sem, (q, zz), x_peer)

    def copy_f(q, side, zz):
        here = block(q, c, x if side == 0 else 1 - x, zz)
        return send(here, here, f_sem, (q, side, zz), c_peer)

    def spread(qs, i, product):
        @pl.when(i < 2 * nz)
        def _():
            for n, q in enumerate(qs):
                part[q, i] = product[:, n * BLOCK : (n + 1) * BLOCK].astype(BF16)
                copy_a(q, i).start()

        @pl.when(i >= 2 * nz)
        def _():
            j = lax.rem(i, nz)
            for n, q in enumerate(qs):
                copy_a(q, i - 2 * nz).wait_recv()
                total = product[:, n * BLOCK : (n + 1) * BLOCK] + got_a[q, i - 2 * nz].astype(F32)

                @pl.when(i < 3 * nz)
                def _():
                    sent_b[q, j] = total.astype(BF16)
                    if n == 0:
                        copy_b(q, j).start()

                @pl.when(i >= 3 * nz)
                def _():
                    kept[q, j] = total

        @pl.when(i == 3 * nz - 1)
        def _():
            for q in qs[1:]:
                for j in range(nz):
                    copy_b(q, j).start()

    def write_out(i):
        here = position(i)
        return pltpu.make_async_copy(blended.at[here], blended_out.at[here], out_sem.at[i])

    dot = functools.partial(jnp.dot, preferred_element_type=F32)

    @pl.loop(0, chunks)
    def _(i):
        slot = lax.rem(i, slots)
        for copy in fetch(i, slot):
            copy.wait()
        value = (stream_m[slot].astype(F32) + stream_g[slot].astype(F32)).astype(BF16)
        blended[position(i)] = value
        spread(near, i, dot(value, lows[0]))

        @pl.when(i + slots < chunks)
        def _():
            for copy in fetch(i + slots, slot):
                copy.start()

    @pl.loop(0, chunks)
    def _(i):
        write_out(i).start()

    def multiply_far(k, start, stop):
        @pl.loop(start // 2, stop // 2)
        def _(pair):
            both = [2 * pair, 2 * pair + 1]
            products = [dot(blended[position(i), pieces[k]], lows[1, pieces[k]]) for i in both]
            for i, product in zip(both, products):
                if k == 0:
                    partial[i] = product
                else:
                    spread(far, i, partial[i] + product)

    def take_b(q, j):
        copy_b(q, j).wait_recv()
        total = kept[q, j] + got_b[q, j].astype(F32)
        if j < nz - 1:
            sent_c[q, j] = total.astype(BF16)
            copy_c(q, j + 1).start()
        else:
            own[q] = total

    def take_c(q):
        total = own[q]
        for d in range(1, nz):
            copy_c(q, d).wait_recv()
            total = total + got_c[q, d - 1].astype(F32)
        left[spot(q), rows_of(c, x, z)] = total.astype(BF16)
        for way in range(2):

            @pl.when(can_send(way, 0))
            def _():
                copy_d(q, way, 0).start()

        copy_e(q, z).start()
        copy_f(q, 0, z).start()

    def landing(q, cc, xx, zz, sems, index):
        here = block(q, cc, xx, zz)
        return send(here, here, sems, index, c_peer)

    def at_distance(k, action):
        @pl.when(z >= k)
        def _():
            action(0, z - k)

        if k > 0:

            @pl.when(z + k < nz)
            def _():
                action(1, z + k)

    def take_d(q, k):
        def arrived(way, zz):
            landing(q, c, x, zz, d_sem, (q, way, k - 1)).wait_recv()
            if k < nz - 1:

                @pl.when(can_send(way, k))
                def _():
                    copy_d(q, way, k).start()

            copy_e(q, zz).start()
            copy_f(q, 0, zz).start()

        at_distance(k, arrived)

    def take_e(q, k):
        def arrived(way, zz):
            landing(q, c, 1 - x, zz, e_sem, (q, zz)).wait_recv()
            copy_f(q, 1, zz).start()

        at_distance(k, arrived)

    def take_f(q):
        for side in range(2):
            for zz in range(nz):
                landing(q, 1 - c, x if side == 0 else 1 - x, zz, f_sem, (q, side, zz)).wait_recv()

    over = (((0,), (0,)), ((), ()))
    step = 2 * size

    def left_rows(g, here):
        return jnp.concatenate([left[g * per_half + n, here] for n in range(per_half)], axis=1)

    steps = blended.shape[0] // step

    def right_part(h, begin, end):
        g = half(h * per_half)
        if begin == 0:
            w[g] = jnp.zeros(w.shape[1:], F32)

        @pl.loop(begin, end)
        def _(k):
            here = pl.ds(pl.multiple_of(k * step, step), step)
            w[g] += lax.dot_general(
                left_rows(g, here), blended[here], over, preferred_element_type=F32
            )

        if end == steps:
            w_out[g] = w[g].astype(BF16)

    def gram_part(index, one, two, cc):
        rows = blended.shape[0] // 2
        here = pl.ds(pl.multiple_of(cc * rows, rows), rows)
        gram[index] += lax.dot_general(
            left_rows(one, here), left_rows(two, here), over, preferred_element_type=F32
        )

    half_columns = columns // 2
    mine = pl.ds(pl.multiple_of(c * half_columns, half_columns), half_columns)
    theirs = pl.ds(pl.multiple_of((1 - c) * half_columns, half_columns), half_columns)

    def copy_g(block_index, index, got_index):
        return send(
            gram.at[block_index, mine], got_gram.at[got_index, mine], g_sem, (index,), y_peer
        )

    gram[...] = jnp.zeros(gram.shape, F32)
    q0, q1, q2, q3 = range(groups)

    def take_all_b(q):
        for j in range(nz):
            take_b(q, j)

    take_all_b(q0)
    take_c(q0)
    copy_l(0).wait_recv()
    multiply_far(0, 0, 2 * nz)
    take_all_b(q1)
    multiply_far(0, 2 * nz, chunks)
    copy_l(1).wait_recv()
    multiply_far(1, 0, 2 * nz)
    take_c(q1)
    multiply_far(1, 2 * nz, chunks)
    take_d(q0, 1)
    take_d(q0, 2)
    take_d(q1, 1)
    take_d(q0, 3)
    for j in range(nz):
        take_b(q2, j)
    take_d(q1, 2)
    take_b(q3, 0)
    take_b(q3, 1)
    take_d(q1, 3)
    take_c(q2)
    take_b(q3, 2)
    take_b(q3, 3)
    take_d(q2, 1)
    take_c(q3)
    for q in near:
        for k in range(nz):
            take_e(q, k)
    take_d(q2, 2)
    for q in near:
        take_f(q)
    right_part(0, 0, 2)
    take_d(q3, 1)
    take_d(q2, 3)
    right_part(0, 2, 4)
    gram_part(place, place, place, 0)
    take_d(q3, 2)
    gram_part(place, place, place, 1)
    copy_g(place, 0, place).start()
    right_part(0, 4, 6)
    take_d(q3, 3)
    right_part(0, 6, steps)
    for q in far:
        for k in range(nz):
            take_e(q, k)
    gram_part(1 - place, 1 - place, 1 - place, c)
    gram_part(2, 0, 1, c)
    for q in far:
        take_f(q)
    gram_part(1 - place, 1 - place, 1 - place, 1 - c)
    gram_part(2, 0, 1, 1 - c)
    copy_g(1 - place, 1, 1 - place).start()
    copy_g(2, 2, 2).start()

    def save_left(g):
        return pltpu.make_async_copy(left.at[g], left_out.at[g], k_sem.at[g])

    for g in range(groups):
        save_left(g).start()
    right_part(1, 0, steps)
    copy_g(place, 0, 1 - place).wait()
    copy_g(1 - place, 1, place).wait()
    copy_g(2, 2, 2).wait()
    gram_out[0, mine, :columns] = gram[0, mine] + got_gram[0, mine]
    gram_out[0, mine, columns:] = gram[2, mine] + got_gram[2, mine]
    gram_out[1, mine, columns:] = gram[1, mine] + got_gram[1, mine]
    gram_out[1, :, :columns] = jnp.zeros((columns, columns), F32)

    def copy_k(here, index):
        return send(gram_out.at[here], gram_out.at[here], g_sem, (index,), c_peer)

    out_k = [copy_k((0, mine), 3), copy_k((1, mine, pl.ds(columns, columns)), 4)]
    for copy in out_k:
        copy.start()

    for g in range(groups):
        save_left(g).wait()

    @pl.loop(0, chunks)
    def _(i):
        write_out(i).wait()

    for k in range(2):
        copy_l(k).wait_send()
    for q in range(groups):

        @pl.loop(0, 2 * nz)
        def _(i):
            copy_a(q, i).wait_send()

        for j in range(nz):
            copy_b(q, j).wait_send()
            copy_e(q, j).wait_send()
            copy_f(q, 0, j).wait_send()
            copy_f(q, 1, j).wait_send()
            if j > 0:
                copy_c(q, j).wait_send()
            if j < nz - 1:
                for way in range(2):

                    @pl.when(can_send(way, j))
                    def _():
                        copy_d(q, way, j).wait_send()

    copy_k((0, theirs), 3).wait_recv()
    copy_k((1, theirs, pl.ds(columns, columns)), 4).wait_recv()
    for copy in out_k:
        copy.wait_send()


def left_stage(nz, momentum, gradient, factor):
    rows, width = momentum.shape
    columns = factor.shape[1]
    size = rows // (4 * nz)
    groups = 2 * columns // BLOCK
    slots = 4
    dma = pltpu.SemaphoreType.DMA
    vmem = pl.BlockSpec(memory_space=pltpu.VMEM)
    anywhere = pl.BlockSpec(memory_space=pl.ANY)
    return pl.pallas_call(
        functools.partial(left_kernel, nz),
        out_shape=(
            jax.ShapeDtypeStruct((rows, width), BF16),
            jax.ShapeDtypeStruct((groups, rows, BLOCK), BF16),
            jax.ShapeDtypeStruct((2, columns, 2 * columns), F32),
            jax.ShapeDtypeStruct((2, columns, width), BF16),
        ),
        in_specs=[anywhere, anywhere, vmem],
        out_specs=(anywhere, anywhere, vmem, vmem),
        scratch_shapes=[
            pltpu.VMEM((2, width, columns), BF16),
            pltpu.VMEM((rows, width), BF16),
            pltpu.VMEM((slots, size, width), BF16),
            pltpu.VMEM((slots, size, width), BF16),
            pltpu.VMEM((groups, 2 * nz, size, BLOCK), BF16),
            pltpu.VMEM((groups, 2 * nz, size, BLOCK), BF16),
            pltpu.VMEM((groups, nz, size, BLOCK), BF16),
            pltpu.VMEM((groups, nz, size, BLOCK), F32),
            pltpu.VMEM((groups, nz, size, BLOCK), BF16),
            pltpu.VMEM((groups, nz - 1, size, BLOCK), BF16),
            pltpu.VMEM((groups, nz - 1, size, BLOCK), BF16),
            pltpu.VMEM((groups, size, BLOCK), F32),
            pltpu.VMEM((4 * nz, size, columns), F32),
            pltpu.VMEM((groups, rows, BLOCK), BF16),
            pltpu.VMEM((2, columns, width), F32),
            pltpu.VMEM((3, columns, columns), F32),
            pltpu.VMEM((3, columns, columns), F32),
            dma((2, slots)),
            dma((4 * nz,)),
            dma((2, 2)),
            dma((2, groups, 2 * nz)),
            dma((2, groups, nz)),
            dma((2, groups, nz - 1)),
            dma((2, groups, 2, nz - 1)),
            dma((2, groups, nz)),
            dma((2, groups, 2, nz)),
            dma((2, 5)),
            dma((groups,)),
        ],
        compiler_params=pltpu.CompilerParams(
            collective_id=0, has_side_effects=True, vmem_limit_bytes=56 << 20
        ),
        name="left",
    )(momentum, gradient, factor)


def right_kernel(
    n, high, low, w, other, left, orthonormal, right_out, normal_out, own_out, right, sums, s_sem
):
    place = lax.axis_index("fsdp")
    t = lax.axis_index("tensor")
    rank, width = right.shape
    columns = own_out.shape[0]
    per_half = columns // BLOCK

    def peer(d):
        return place, lax.rem(t + d, n)

    def copy(d):
        return pltpu.make_async_remote_copy(
            src_ref=sums.at[0],
            dst_ref=sums.at[d],
            send_sem=s_sem.at[0, d],
            recv_sem=s_sem.at[1, d],
            device_id=peer(d),
            device_id_type=MESH,
        )

    barrier = pltpu.get_barrier_semaphore()

    @pl.loop(1, n)
    def _(d):
        pl.semaphore_signal(barrier, inc=1, device_id=peer(d), device_id_type=MESH)

    dot = functools.partial(jnp.dot, preferred_element_type=F32)
    squares = jnp.zeros((rank, BLOCK), F32)
    for start in range(0, width, 2 * BLOCK):
        here = slice(start, start + 2 * BLOCK)
        total = w[:, here].astype(F32) + other[:, here].astype(F32)
        w_high = total.astype(BF16)
        w_low = (total - w_high.astype(F32)).astype(BF16)
        value = dot(high[...], w_high) + dot(high[...], w_low) + dot(low[...], w_high)
        right[:, here] = value
        value = value * value
        squares = squares + value[:, :BLOCK] + value[:, BLOCK:]
    sums[0] = jnp.sum(squares.T, axis=0, keepdims=True)
    pl.semaphore_wait(barrier, n - 1)

    @pl.loop(1, n)
    def _(d):
        copy(d).start()

    right_out[...] = right[...].astype(BF16)
    size = 256
    across = (((1,), (1,)), ((), ()))

    @pl.loop(0, left.shape[1] // size)
    def _(i):
        here = pl.ds(pl.multiple_of(i * size, size), size)
        total = None
        for g in range(2):
            rows = jnp.concatenate([left[g * per_half + n, here] for n in range(per_half)], axis=1)
            for piece in (high, low):
                term = lax.dot_general(
                    rows,
                    piece[:, g * columns : (g + 1) * columns],
                    across,
                    preferred_element_type=F32,
                )
                total = term if total is None else total + term
        orthonormal[here] = total.astype(BF16)

    @pl.loop(1, n)
    def _(d):
        copy(d).wait()

    square_sums = sums[0]
    for d in range(1, n):
        square_sums = square_sums + sums[d]
    inverse = jnp.broadcast_to(lax.rsqrt(square_sums + epsilon), (BLOCK, rank)).T
    for start in range(0, width, BLOCK):
        here = slice(start, start + BLOCK)
        right[:, here] = right[:, here] * inverse
    normal_out[...] = right[...].astype(BF16)
    own_out[...] = right[pl.ds(pl.multiple_of(place * columns, columns), columns)]


def right_stage(n, high, low, w, other, left):
    rank, width = w.shape
    rows = left.shape[1]
    columns = rank // 2
    vmem = pl.BlockSpec(memory_space=pltpu.VMEM)
    return pl.pallas_call(
        functools.partial(right_kernel, n),
        out_shape=(
            jax.ShapeDtypeStruct((rows, rank), BF16),
            jax.ShapeDtypeStruct((rank, width), BF16),
            jax.ShapeDtypeStruct((rank, width), BF16),
            jax.ShapeDtypeStruct((columns, width), F32),
        ),
        in_specs=[vmem] * 5,
        out_specs=(vmem,) * 4,
        scratch_shapes=[
            pltpu.VMEM((rank, width), F32),
            pltpu.VMEM((n, 1, rank), F32),
            pltpu.SemaphoreType.DMA((2, n)),
        ],
        compiler_params=pltpu.CompilerParams(
            collective_id=1, has_side_effects=True, vmem_limit_bytes=32 << 20
        ),
        cost_estimate=pl.CostEstimate(flops=8_000_000_000, bytes_accessed=16 << 20, transcendentals=0),
        name="right",
    )(high, low, w, other, left)


def output_kernel(scale, orthonormal, blended, right, normal, own, momentum_out, update_out, factor_out):
    product = jnp.dot(orthonormal[...], right[...], preferred_element_type=F32)
    momentum_out[...] = (blended[...].astype(F32) - (1.0 - decay_rate) * product).astype(BF16)
    stepped = jnp.dot(orthonormal[...], normal[...], preferred_element_type=F32)
    update_out[...] = (stepped * scale).astype(BF16)
    factor_out[...] = own[...].T


def output_stage(scale, orthonormal, blended, right, normal, own):
    rows, width = blended.shape
    rank = orthonormal.shape[1]
    columns = own.shape[0]
    size = 256
    last = width // BLOCK - 1
    whole = pl.BlockSpec((rank, width), lambda i: (0, 0), pipeline_mode=pl.Buffered(1))
    chunk = pl.BlockSpec((size, width), lambda i: (i, 0))
    return pl.pallas_call(
        functools.partial(output_kernel, scale),
        grid=(rows // size,),
        out_shape=(jax.ShapeDtypeStruct((rows, width), BF16),) * 2
        + (jax.ShapeDtypeStruct((width, columns), F32),),
        in_specs=[
            pl.BlockSpec((size, rank), lambda i: (i, 0)),
            chunk,
            whole,
            whole,
            pl.BlockSpec((columns, BLOCK), lambda i: (0, jnp.minimum(i, last))),
        ],
        out_specs=(chunk, chunk, pl.BlockSpec((BLOCK, columns), lambda i: (jnp.minimum(i, last), 0))),
        compiler_params=pltpu.CompilerParams(
            dimension_semantics=("arbitrary",), vmem_limit_bytes=40 << 20
        ),
        name="outputs",
    )(orthonormal, blended, right, normal, own)


def paired(halves, spread, momentum, gradient, factor):
    whole_rows = momentum.shape[0] * halves
    whole_columns = momentum.shape[1] * spread
    rank = factor.shape[1] * halves

    blended, left, gram, w = left_stage(spread // 4, momentum, gradient, factor)
    w = w.reshape(rank, w.shape[2])
    other = lax.ppermute(w, "fsdp", [(0, 1), (1, 0)])
    high, low = inverse_of_lower(gram.reshape(rank, rank))
    orthonormal, right, normal, own = right_stage(spread, high, low, w, other, left)
    scale = (whole_rows * whole_columns / rank) ** 0.5
    new_momentum, update, new_factor = output_stage(scale, orthonormal, blended, right, normal, own)
    return (new_momentum, new_factor, update)


def general(halves, spread, momentum, gradient, factor):
    whole_rows = momentum.shape[0] * halves
    whole_columns = momentum.shape[1] * spread
    own_rank = factor.shape[1]
    rank = own_rank * halves
    place = lax.axis_index("fsdp")

    blended = (momentum.astype(jnp.float32) + gradient.astype(jnp.float32)).astype(jnp.bfloat16)
    lowered = lax.all_gather(factor.astype(jnp.bfloat16), "fsdp", axis=1, tiled=True)
    part = jnp.dot(blended, lowered, preferred_element_type=jnp.float32).astype(jnp.bfloat16)
    rows = lax.psum_scatter(part, "tensor", scatter_dimension=0, tiled=True)

    gram = lax.psum(
        lax.dot_general(rows, rows, (((0,), (0,)), ((), ())), preferred_element_type=jnp.float32),
        ("fsdp", "tensor"),
    )
    left = lax.all_gather(rows, "tensor", axis=0, tiled=True)
    high, low = inverse_of_lower(gram)
    across = (((1,), (1,)), ((), ()))
    orthonormal = (
        lax.dot_general(left, high, across, preferred_element_type=jnp.float32)
        + lax.dot_general(left, low, across, preferred_element_type=jnp.float32)
    ).astype(jnp.bfloat16)

    share = lax.dot_general(
        orthonormal, blended, (((0,), (0,)), ((), ())), preferred_element_type=jnp.float32
    ).astype(jnp.bfloat16)
    right = lax.psum(share, "fsdp").astype(jnp.float32)
    square_sums = butterfly(jnp.sum(right * right, axis=1), "tensor", spread)
    inverse = lax.rsqrt(square_sums + epsilon)
    normal = right * inverse[:, None]
    own_factor = lax.dynamic_slice_in_dim(normal, place * own_rank, own_rank, axis=0).T
    product = jnp.dot(orthonormal, right.astype(jnp.bfloat16), preferred_element_type=jnp.float32)
    new_momentum = (blended.astype(jnp.float32) - (1.0 - decay_rate) * product).astype(jnp.bfloat16)
    stepped = jnp.dot(orthonormal, normal.astype(jnp.bfloat16), preferred_element_type=jnp.float32)
    scale = jnp.sqrt(jnp.float32(whole_rows * whole_columns / rank))
    update = (stepped * scale).astype(jnp.bfloat16)
    return (new_momentum, own_factor, update)


def solution(mesh):
    halves, spread = mesh.shape["fsdp"], mesh.shape["tensor"]

    def body(momentum, gradient, factor):
        rows, width = momentum.shape
        fits = rows % (2 * spread * BLOCK) == 0 and width % (2 * BLOCK) == 0
        fits = fits and factor.shape[1] == 2 * BLOCK and width // BLOCK <= rows // (2 * BLOCK)
        paired_mesh = halves == 2 and spread == 16
        on_device = paired if paired_mesh and fits else general
        return on_device(halves, spread, momentum, gradient, factor)

    return jax.shard_map(
        body,
        mesh=mesh,
        in_specs=(P("fsdp", "tensor"), P("fsdp", "tensor"), P("tensor", "fsdp")),
        out_specs=(P("fsdp", "tensor"), P("tensor", "fsdp"), P("fsdp", "tensor")),
        check_vma=False,
    )
```
